32 devices in a mesh: dp: 8 (over y, x, core), mp: 4 (over z).
Axes of the slice: x: 2, y: 2, z: 4, core: 2. Of those that a mesh axis runs over, the one named last changes fastest.
Arguments:
- hidden_in: float32 [16384, 768], P(('dp', 'mp')), may hold values from -6 to 6
- first_values: bfloat16 [16384, 384], P('dp', 'mp'), may hold values from -6 to 6
- first_length: int32 [8], P('dp'), may hold values from 1024 to 2048, as said below
- pre_gain: float32 [768], replicated, may hold values from 0.25 to 1.75
- pre_shift: float32 [768], replicated, may hold values from -1.75 to 1.75
- w_query: bfloat16 [768, 768], P(None, 'mp'), may hold values from -0.21875 to 0.21875
- b_query: float32 [768], P('mp'), may hold values from -3 to 3
- w_key: bfloat16 [768, 768], P(None, 'mp'), may hold values from -0.21875 to 0.21875
- w_value: bfloat16 [768, 384], P(None, 'mp'), may hold values from -0.21875 to 0.21875
- b_value: float32 [384], P('mp'), may hold values from -3 to 3
- w_out: bfloat16 [768, 768], P('mp'), may hold values from -1.75 to 1.75
- b_out: float32 [768], replicated, may hold values from -3 to 3
- mid_gain: float32 [768], replicated, may hold values from 0.25 to 1.75
- mid_shift: float32 [768], replicated, may hold values from -1.75 to 1.75
- w_up: bfloat16 [768, 3072], P(None, 'mp'), may hold values from -0.21875 to 0.21875
- b_up: float32 [3072], P('mp'), may hold values from -3 to 3
- w_down: bfloat16 [3072, 768], P('mp'), may hold values from -0.109375 to 0.109375
- b_down: float32 [768], replicated, may hold values from -3 to 3
- grad_out: float32 [16384, 768], P(('dp', 'mp')), may hold values from -6 to 6
Outputs:
- layer_out: float32 [16384, 768], P(('dp', 'mp'))
- grad_in: float32 [16384, 768], P(('dp', 'mp'))
- grad_first_values: float32 [16384, 384], P('dp', 'mp')
- grad_pre_gain: float32 [768], replicated
- grad_pre_shift: float32 [768], replicated
- grad_w_query: float32 [768, 768], P(None, 'mp')
- grad_b_query: float32 [768], P('mp')
- grad_w_key: float32 [768, 768], P(None, 'mp')
- grad_w_value: float32 [768, 384], P(None, 'mp')
- grad_b_value: float32 [384], P('mp')
- grad_w_out: float32 [768, 768], P('mp')
- grad_b_out: float32 [768], replicated
- grad_mid_gain: float32 [768], replicated
- grad_mid_shift: float32 [768], replicated
- grad_w_up: float32 [768, 3072], P(None, 'mp')
- grad_b_up: float32 [3072], P('mp')
- grad_w_down: float32 [3072, 768], P('mp')
- grad_b_down: float32 [768], replicated
The draws below stay inside these ranges and needn't reach their ends.
Inputs may be any that keep to these rules, and one draw needn't show every extreme that they name: `first_length`: each entry is 2048 / 2 (two documents in the block) or 2048 (one document); half of the entries take each value.
All inputs are finite; a program needn't handle non-finite values.
Results may differ from the reference program's by a relative error of at most 0.02.
Values may be sent and summed in bfloat16 or wider, within the bound.
A program may use at most 192 MiB of HBM per device.

```python
import jax
import jax.numpy as jnp
from jax import lax

D = 768
HEADS = 12
HEAD_DIM = 64
FF = 3072
FRESH = 6
TOK_DEV = 2048
TOKENS = 16384
N_DP = 8


def draw_first_length(key, part):
    order = jax.random.permutation(key, N_DP)
    return jnp.where(order < N_DP // 2, TOK_DEV, TOK_DEV // 2).astype(jnp.int32)


def level_of(own_key, dims, shards, least, largest):
    loudness, own = 1.0, jax.random.fold_in(own_key, 6)
    for dim, parts in shards:
        draws = jnp.exp(jax.random.uniform(jax.random.fold_in(own, dim), (parts,), jnp.float32, least / len(shards), largest / len(shards)))
        loudness = loudness * jnp.repeat(draws, dims[dim] // parts).reshape([-1 if axis == dim else 1 for axis in range(len(dims))])
    return loudness


def gaussian(rng, dims, scale, reach, pieces=(), held_as=jnp.bfloat16):
    array = scale * jax.random.normal(rng, dims, jnp.float32)
    if pieces:
        array = array * level_of(rng, dims, pieces, -0.22, 0.18)
    return jnp.clip(array, -reach, reach).astype(held_as)


def setup_inputs(seed: int = 0) -> dict:
    arg_keys = jax.random.split(jax.random.key(seed), 20)
    return {
        "hidden_in": gaussian(arg_keys[0], (TOKENS, D), 1.0, 6.0, ((0, 32),), jnp.float32),
        "first_values": gaussian(arg_keys[1], (TOKENS, FRESH * HEAD_DIM), 1.0, 6.0, ((0, 8), (1, 4))),
        "first_length": draw_first_length(jax.random.fold_in(arg_keys[19], 71), 0),
        "pre_gain": jnp.clip(1.0 + 0.15 * jax.random.normal(arg_keys[3], (D,), jnp.float32), 0.25, 1.75),
        "pre_shift": gaussian(arg_keys[4], (D,), 0.3, 1.75, (), jnp.float32),
        "w_query": gaussian(arg_keys[5], (D, D), D ** -0.5, 0.21875, ((1, 4),)),
        "b_query": gaussian(arg_keys[6], (D,), 0.5, 3.0, ((0, 4),), jnp.float32),
        "w_key": gaussian(arg_keys[7], (D, D), D ** -0.5, 0.21875, ((1, 4),)),
        "w_value": gaussian(arg_keys[8], (D, FRESH * HEAD_DIM), D ** -0.5, 0.21875, ((1, 4),)),
        "b_value": gaussian(arg_keys[9], (FRESH * HEAD_DIM,), 0.5, 3.0, ((0, 4),), jnp.float32),
        "w_out": gaussian(arg_keys[10], (D, D), (max(D // 64, 1)) ** -0.5, 1.75, ((0, 4),)),
        "b_out": gaussian(arg_keys[11], (D,), 0.5, 3.0, (), jnp.float32),
        "mid_gain": jnp.clip(1.0 + 0.15 * jax.random.normal(arg_keys[12], (D,), jnp.float32), 0.25, 1.75),
        "mid_shift": gaussian(arg_keys[13], (D,), 0.3, 1.75, (), jnp.float32),
        "w_up": gaussian(arg_keys[14], (D, FF), D ** -0.5, 0.21875, ((1, 4),)),
        "b_up": gaussian(arg_keys[15], (FF,), 0.5, 3.0, ((0, 4),), jnp.float32),
        "w_down": gaussian(arg_keys[16], (FF, D), FF ** -0.5, 0.109375, ((0, 4),)),
        "b_down": gaussian(arg_keys[17], (D,), 0.5, 3.0, (), jnp.float32),
        "grad_out": gaussian(arg_keys[18], (TOKENS, D), 1.0, 6.0, ((0, 32),), jnp.float32),
    }


@jax.custom_vjp
def low(v):
    return lax.optimization_barrier(v.astype(jnp.bfloat16)).astype(jnp.float32)

@jax.custom_vjp
def low_back(v):
    return v

def low_keep(v):
    return (low(v), None)

def low_pass(kept, grad):
    return (grad,)

def back_keep(v):
    return (v, None)

def back_low(kept, grad):
    return (low(grad),)
low.defvjp(low_keep, low_pass)
low_back.defvjp(back_keep, back_low)
EPSILON = 1e-05

def layer_norm(values, gain, shift):
    center = values - lax.optimization_barrier(jnp.mean(values, -1, keepdims=True))
    spread = lax.optimization_barrier(jnp.mean(center * center, -1, keepdims=True))
    return center * lax.rsqrt(spread + EPSILON) * gain + shift

def gelu_tanh(values):
    return 0.5 * values * (1.0 + jnp.tanh(0.7978845608028654 * (values + 0.044715 * values * values * values)))

def matmul(left, right):
    return jnp.dot(left, right, precision=lax.Precision.HIGHEST, preferred_element_type=jnp.float32)

def group_layer(params, hidden_in, first_values, first_length):
    pre_gain, pre_shift, w_query, b_query, w_key, w_value, b_value, w_out, b_out, mid_gain, mid_shift, w_up, b_up, w_down, b_down = params
    length = hidden_in.shape[0]
    normed = low(layer_norm(hidden_in, pre_gain, pre_shift))
    queries = low(low_back(matmul(normed, w_query) + b_query))
    keys_all = low(low_back(matmul(normed, w_key)))
    fresh_values = low(low_back(matmul(normed, w_value) + b_value))
    values_all = jnp.concatenate([fresh_values, first_values], 1)
    heads_query = queries.reshape(length, HEADS, HEAD_DIM)
    heads_key = keys_all.reshape(length, HEADS, HEAD_DIM)
    heads_value = values_all.reshape(length, HEADS, HEAD_DIM)
    position = jnp.arange(length, dtype=jnp.int32)
    second = position >= first_length
    allowed = (position[None, :] <= position[:, None]) & (second[None, :] == second[:, None])
    scores = low_back(jnp.einsum('qhd,khd->hqk', heads_query, heads_key, precision=lax.Precision.HIGHEST) * HEAD_DIM ** (-0.5))
    scores = jnp.where(allowed[None], scores, -1e+30)
    row_max = lax.optimization_barrier(jnp.max(scores, -1, keepdims=True))
    exponent = jnp.exp(scores - row_max)
    probabilities = low(exponent / lax.optimization_barrier(jnp.sum(exponent, -1, keepdims=True)))
    context = jnp.einsum('hqk,khd->qhd', probabilities, heads_value, precision=lax.Precision.HIGHEST).reshape(length, HEADS * HEAD_DIM)
    context = low(low_back(context))
    attended = low_back(matmul(context, w_out) + b_out)
    middle = hidden_in + attended
    normed_mid = low(layer_norm(middle, mid_gain, mid_shift))
    up_values = low_back(matmul(normed_mid, w_up) + b_up)
    activated = low(gelu_tanh(up_values))
    return middle + low_back(matmul(activated, w_down) + b_down)

def reference(hidden_in, first_values, first_length, pre_gain, pre_shift, w_query, b_query, w_key, w_value, b_value, w_out, b_out, mid_gain, mid_shift, w_up, b_up, w_down, b_down, grad_out):
    params = tuple((item.astype(jnp.float32) for item in (pre_gain, pre_shift, w_query, b_query, w_key, w_value, b_value, w_out, b_out, mid_gain, mid_shift, w_up, b_up, w_down, b_down)))
    blocks_in = hidden_in.astype(jnp.float32).reshape(N_DP, TOK_DEV, D)
    blocks_first = first_values.astype(jnp.float32).reshape(N_DP, TOK_DEV, FRESH * HEAD_DIM)
    blocks_grad = grad_out.astype(jnp.float32).reshape(N_DP, TOK_DEV, D)
    lengths = first_length.astype(jnp.int32)

    def forward(weights, inputs, firsts):

        def one_group(items):
            return group_layer(weights, items[0], items[1], items[2])
        return lax.map(jax.checkpoint(one_group), (inputs, firsts, lengths))
    result, pullback = jax.vjp(forward, params, blocks_in, blocks_first)
    grad_params, grad_input, grad_first = pullback(blocks_grad)
    return (result.reshape(TOKENS, D), grad_input.reshape(TOKENS, D), grad_first.reshape(TOKENS, FRESH * HEAD_DIM), grad_params[0], grad_params[1], grad_params[2], grad_params[3], grad_params[4], grad_params[5], grad_params[6], grad_params[7], grad_params[8], grad_params[9], grad_params[10], grad_params[11], grad_params[12], grad_params[13], grad_params[14])
```

```python
import functools

import jax
import jax.numpy as jnp
from jax import lax
from jax.experimental import pallas as pl
from jax.experimental.pallas import tpu as pltpu
from jax.sharding import PartitionSpec as P

EPSILON = 1e-05
HEAD = 64
BLK = 256
LOG2E = 1.4426950408889634
LN2 = 0.6931471805599453


def nn(left, right):
    return lax.dot_general(left, right, (((1,), (0,)), ((), ())), preferred_element_type=jnp.float32)


def nt(left, right):
    return lax.dot_general(left, right, (((1,), (1,)), ((), ())), preferred_element_type=jnp.float32)


def tn(left, right):
    return lax.dot_general(left, right, (((0,), (0,)), ((), ())), preferred_element_type=jnp.float32)


def causal_mask(size):
    keys = lax.broadcasted_iota(jnp.int32, (size, size), 0)
    rows = lax.broadcasted_iota(jnp.int32, (size, size), 1)
    return keys <= rows


def forward_kernel(heads, factor, first_ref, q_ref, k_ref, v_ref, out_ref, lse_ref):
    row = pl.program_id(0)
    split = first_ref[0] // BLK
    lowest = jnp.where(row >= split, split, 0)
    query = [q_ref[h * HEAD : (h + 1) * HEAD, :] for h in range(heads)]

    def block(col, carry, masked):
        cols = pl.ds(pl.multiple_of(col * BLK, BLK), BLK)
        result = []
        for h in range(heads):
            run_max, run_sum, running = carry[h]
            band = slice(h * HEAD, (h + 1) * HEAD)
            scores = tn(k_ref[band, cols], query[h])
            if masked:
                scores = jnp.where(causal_mask(BLK), scores, -1e30)
            new_max = jnp.maximum(run_max, jnp.max(scores, 0, keepdims=True))
            change = jnp.exp2((run_max - new_max) * factor)
            weights = jnp.exp2((scores - new_max) * factor)
            run_sum = run_sum * change + jnp.sum(weights, 0, keepdims=True)
            running = running * change + nn(v_ref[band, cols], weights.astype(jnp.bfloat16))
            result.append((new_max, run_sum, running))
        return tuple(result)

    start = tuple(
        (
            jnp.full((1, BLK), -1e30, jnp.float32),
            jnp.zeros((1, BLK), jnp.float32),
            jnp.zeros((HEAD, BLK), jnp.float32),
        )
        for _ in range(heads)
    )
    start = block(row, start, True)
    final = lax.fori_loop(lowest, row, lambda col, carry: block(col, carry, False), start)
    for h in range(heads):
        run_max, run_sum, running = final[h]
        out_ref[0, h * HEAD : (h + 1) * HEAD, :] = (running / run_sum).astype(jnp.bfloat16)
        lse_ref[h : h + 1, :] = run_max * factor + jnp.log2(run_sum)


def attend_forward(first_length, queries, keys, values, parts):
    width, count = queries.shape
    heads = width // HEAD
    blocks = count // BLK
    chunk = count // parts
    per = chunk // BLK
    factor = HEAD ** (-0.5) * LOG2E
    spec_all = pl.BlockSpec((width, count), lambda i: (0, 0))
    return pl.pallas_call(
        functools.partial(forward_kernel, heads, factor),
        grid=(blocks,),
        in_specs=[
            pl.BlockSpec(memory_space=pltpu.SMEM),
            pl.BlockSpec((width, BLK), lambda i: (0, i)),
            spec_all,
            spec_all,
        ],
        out_specs=[
            pl.BlockSpec((1, width, BLK), lambda i: (i // per, 0, i % per)),
            pl.BlockSpec((8, BLK), lambda i: (0, i)),
        ],
        out_shape=[
            jax.ShapeDtypeStruct((parts, width, chunk), jnp.bfloat16),
            jax.ShapeDtypeStruct((8, count), jnp.float32),
        ],
        cost_estimate=pl.CostEstimate(
            flops=4 * count * count * 256 * heads, bytes_accessed=8 * width * count, transcendentals=0
        ),
        name="attend_forward",
    )(first_length, queries, keys, values)


def backward_kernel(
    heads, factor, total, per, first_ref, q_ref, k_ref, v_ref, go_ref, o_ref, lse_ref,
    gq_ref, gk_ref, gv_ref, gq_sum, delta_ref,
):
    col = pl.program_id(0)
    split = first_ref[0] // BLK
    last = jnp.where(col < split, split, total)

    @pl.when(col == 0)
    def _():
        gq_sum[...] = jnp.zeros_like(gq_sum)
        for part in range(total // per):
            for h in range(heads):
                band = slice(h * HEAD, (h + 1) * HEAD)
                both = go_ref[part, band, :].astype(jnp.float32) * o_ref[part, band, :].astype(jnp.float32)
                delta_ref[h : h + 1, part * per * BLK : (part + 1) * per * BLK] = jnp.sum(
                    both, 0, keepdims=True
                )

    bands = [slice(h * HEAD, (h + 1) * HEAD) for h in range(heads)]
    key = [k_ref[band, :] for band in bands]
    value = [v_ref[band, :] for band in bands]

    def block(row, carry, masked):
        rows = pl.ds(pl.multiple_of(row * BLK, BLK), BLK)
        inner = pl.ds(pl.multiple_of((row % per) * BLK, BLK), BLK)
        result = []
        for h in range(heads):
            grad_k, grad_v = carry[h]
            query = q_ref[bands[h], rows]
            grad_o = go_ref[row // per, bands[h], inner]
            scores = tn(key[h], query)
            probs = jnp.exp2(scores * factor - lse_ref[h : h + 1, rows])
            if masked:
                probs = jnp.where(causal_mask(BLK), probs, 0.0)
            grad_p = tn(value[h], grad_o)
            grad_s = (probs * (grad_p - delta_ref[h : h + 1, rows])).astype(jnp.bfloat16)
            grad_v = grad_v + nt(grad_o, probs.astype(jnp.bfloat16))
            grad_k = grad_k + nt(query, grad_s)
            gq_sum[bands[h], rows] += nn(key[h], grad_s)
            result.append((grad_k, grad_v))
        return tuple(result)

    zero = jnp.zeros((HEAD, BLK), jnp.float32)
    start = block(col, tuple((zero, zero) for _ in range(heads)), True)
    final = lax.fori_loop(col + 1, last, lambda row, carry: block(row, carry, False), start)
    scale = HEAD ** (-0.5)
    for h in range(heads):
        gk_ref[bands[h], :] = (final[h][0] * scale).astype(jnp.bfloat16)
        gv_ref[bands[h], :] = final[h][1].astype(jnp.bfloat16)

    @pl.when(col == total - 1)
    def _():
        gq_ref[...] = (gq_sum[...] * scale).astype(jnp.bfloat16)


def attend_backward(first_length, queries, keys, values, grad_context, context, lse):
    width, count = queries.shape
    heads = width // HEAD
    blocks = count // BLK
    parts, _, chunk = context.shape
    per = chunk // BLK
    factor = HEAD ** (-0.5) * LOG2E
    whole = lambda shape: pl.BlockSpec(shape, lambda i: (0,) * len(shape))
    one = pl.BlockSpec((width, BLK), lambda i: (0, i))
    flat = jax.ShapeDtypeStruct((width, count), jnp.bfloat16)
    return pl.pallas_call(
        functools.partial(backward_kernel, heads, factor, blocks, per),
        grid=(blocks,),
        in_specs=[
            pl.BlockSpec(memory_space=pltpu.SMEM),
            whole((width, count)),
            one,
            one,
            whole((parts, width, chunk)),
            whole((parts, width, chunk)),
            whole((8, count)),
        ],
        out_specs=[whole((width, count)), one, one],
        out_shape=[flat, flat, flat],
        scratch_shapes=[pltpu.VMEM((width, count), jnp.float32), pltpu.VMEM((8, count), jnp.float32)],
        cost_estimate=pl.CostEstimate(
            flops=10 * count * count * 256 * heads, bytes_accessed=14 * width * count, transcendentals=0
        ),
        name="attend_backward",
    )(first_length, queries, keys, values, grad_context, context, lse)


def layer_norm(values, gain, shift):
    center = values - jnp.mean(values, -1, keepdims=True)
    spread = jnp.mean(center * center, -1, keepdims=True)
    return center * lax.rsqrt(spread + EPSILON) * gain + shift


def gelu_tanh(values):
    return (
        0.5
        * values
        * (1.0 + jnp.tanh(0.7978845608028654 * (values + 0.044715 * values * values * values)))
    )


def shards(
    hidden_in,
    first_values,
    first_length,
    pre_gain,
    pre_shift,
    w_query,
    b_query,
    w_key,
    w_value,
    b_value,
    w_out,
    b_out,
    mid_gain,
    mid_shift,
    w_up,
    b_up,
    w_down,
    b_down,
    grad_out,
):
    bf16, f32 = jnp.bfloat16, jnp.float32
    rank = lax.axis_index("mp")
    parts = lax.axis_size("mp")
    copies = lax.axis_size("dp")
    copy = lax.axis_index("dp")
    width = w_query.shape[1]
    model = w_query.shape[0]
    hidden = w_up.shape[1]
    piece = w_value.shape[1]
    used = width // piece
    fresh_ranks = parts // used

    normed_local = layer_norm(hidden_in, pre_gain, pre_shift).astype(bf16)
    normed = lax.all_gather(normed_local, "mp", axis=0, tiled=True)
    count = normed.shape[0]
    chunk = count // parts

    fresh_moves, first_moves = [], []
    for which in range(used):
        fresh_moves.append([(d * used + which, d) for d in range(fresh_ranks)])
        first_moves.append([(d * used + which, d + fresh_ranks) for d in range(parts - fresh_ranks)])
    is_fresh = rank < fresh_ranks
    first_t = first_values.T
    first_own = jnp.concatenate([lax.ppermute(first_t, "mp", m) for m in first_moves], 0)
    w_value_own = jnp.concatenate([lax.ppermute(w_value, "mp", m) for m in fresh_moves], 1)
    b_value_row = b_value[None]
    b_value_own = jnp.concatenate([lax.ppermute(b_value_row, "mp", m) for m in fresh_moves], 1)[0]

    up_rows, out_rows = model // copies, width // copies
    mine = jnp.concatenate(
        [
            lax.dynamic_slice_in_dim(w_up, copy * up_rows, up_rows, 0),
            lax.dynamic_slice_in_dim(w_down, copy * (hidden // copies), hidden // copies, 0),
            lax.dynamic_slice_in_dim(w_out, copy * out_rows, out_rows, 0),
        ],
        0,
    )
    ranked = lax.all_gather(mine, "mp", axis=0)
    gathered = lax.all_gather(ranked, "dp", axis=0)
    down_rows = hidden // copies

    def whole(start, size):
        part = gathered[:, :, start : start + size]
        return jnp.transpose(part, (1, 0, 2, 3)).reshape(parts, copies * size, model)

    up_all = whole(0, up_rows)
    down_all = whole(up_rows, down_rows)
    out_all = whole(up_rows + down_rows, out_rows).reshape(parts * width, model)
    b_up_all = lax.all_gather(b_up, "mp", axis=0)

    queries = (tt(w_query, normed) + b_query[:, None]).astype(bf16)
    keys = tt(w_key, normed).astype(bf16)
    fresh = (tt(w_value_own, normed) + b_value_own[:, None]).astype(bf16)
    values = jnp.where(is_fresh, fresh, first_own)
    context, lse = attend_forward(first_length, queries, keys, values, parts)
    context_rows = lax.all_to_all(context, "mp", 0, 0, tiled=True).reshape(parts * width, chunk)
    middle = hidden_in + (tn(context_rows, out_all) + b_out)
    normed_mid = layer_norm(middle, mid_gain, mid_shift).astype(bf16)
    up_values = (
        lax.dot_general(
            normed_mid, up_all, (((1,), (1,)), ((), ())), preferred_element_type=f32
        )
        + b_up_all[None]
    )
    activated = gelu_tanh(up_values).astype(bf16)
    layer_out = middle + (
        lax.dot_general(
            activated, down_all, (((1, 2), (0, 1)), ((), ())), preferred_element_type=f32
        )
        + b_down
    )
    grad_down = grad_out.astype(bf16)
    grad_b_down = jnp.sum(grad_down.astype(f32), 0)
    grad_w_down = lax.dot_general(
        activated, grad_down, (((0,), (0,)), ((), ())), preferred_element_type=f32
    ).astype(bf16)
    grad_activated = lax.dot_general(
        grad_down, down_all, (((1,), (2,)), ((), ())), preferred_element_type=f32
    )
    _, gelu_pull = jax.vjp(gelu_tanh, up_values)
    grad_up = gelu_pull(grad_activated)[0].astype(bf16)
    grad_b_up = jnp.sum(grad_up.astype(f32), 0)
    grad_w_up = jnp.stack([tn(normed_mid, grad_up[:, j]) for j in range(parts)], 0).astype(bf16)
    grad_normed_mid = lax.dot_general(
        grad_up, up_all, (((1, 2), (0, 2)), ((), ())), preferred_element_type=f32
    )
    _, mid_pull = jax.vjp(layer_norm, middle, mid_gain, mid_shift)
    grad_mid_part, grad_mid_gain, grad_mid_shift = mid_pull(grad_normed_mid)
    grad_middle = grad_out + grad_mid_part
    grad_attn = grad_middle.astype(bf16)
    grad_b_out = jnp.sum(grad_attn.astype(f32), 0)
    grad_context_rows = nt(out_all, grad_attn).astype(bf16).reshape(parts, width, chunk)
    grad_context = lax.all_to_all(grad_context_rows, "mp", 0, 0, tiled=True)
    grad_w_out = nn(context_rows, grad_attn).astype(bf16).reshape(parts, width, model)

    def scatter(full, rows):
        return jnp.transpose(full.reshape(parts, copies, rows, model), (1, 0, 2, 3))

    partial = jnp.concatenate(
        [scatter(grad_w_up, up_rows), scatter(grad_w_down, down_rows), scatter(grad_w_out, out_rows)], 2
    )
    rows_each = partial.shape[2]
    reduced = lax.psum_scatter(
        partial.reshape(copies * parts * rows_each, model), "dp", scatter_dimension=0, tiled=True
    )
    reduced = lax.psum_scatter(reduced, "mp", scatter_dimension=0, tiled=True)
    summed = lax.all_gather(reduced, "dp", axis=0, tiled=True).reshape(copies, rows_each, model)

    def own(start, size):
        return summed[:, start : start + size].reshape(copies * size, model).astype(f32)

    g_w_up = own(0, up_rows)
    g_w_down = own(up_rows, down_rows)
    g_w_out = own(up_rows + down_rows, out_rows)

    grad_q, grad_k, grad_v = attend_backward(
        first_length, queries, keys, values, grad_context, context, lse
    )
    back_fresh = [[(d, s) for s, d in m] for m in fresh_moves]
    back_first = [[(d, s) for s, d in m] for m in first_moves]
    grad_first_t = sum(
        lax.ppermute(grad_v[i * piece : (i + 1) * piece], "mp", m) for i, m in enumerate(back_first)
    )
    grad_first = grad_first_t.T.astype(f32)
    grad_fresh = jnp.where(is_fresh, grad_v, jnp.zeros_like(grad_v))
    grad_normed = lax.psum_scatter(
        (tt_rows(grad_q, w_query) + tt_rows(grad_k, w_key) + tt_rows(grad_fresh, w_value_own)).astype(
            bf16
        ),
        "mp",
        scatter_dimension=0,
        tiled=True,
    ).astype(f32)
    g_q = tn_t(normed, grad_q)
    g_k = tn_t(normed, grad_k)
    g_v = tn_t(normed, grad_fresh).astype(bf16)
    g_v = sum(
        lax.ppermute(g_v[:, i * piece : (i + 1) * piece], "mp", m) for i, m in enumerate(back_fresh)
    )
    grad_b_query = jnp.sum(grad_q.astype(f32), 1)
    sums_v = jnp.sum(grad_fresh.astype(f32), 1)[None]
    grad_b_value = sum(
        lax.ppermute(sums_v[:, i * piece : (i + 1) * piece], "mp", m) for i, m in enumerate(back_fresh)
    )[0]
    grad_w_query, grad_w_key, grad_w_value = lax.psum((g_q.astype(bf16), g_k.astype(bf16), g_v), "dp")
    grad_b_query, grad_b_value = lax.psum((grad_b_query, grad_b_value), "dp")
    _, pre_pull = jax.vjp(layer_norm, hidden_in, pre_gain, pre_shift)
    grad_pre_part, grad_pre_gain, grad_pre_shift = pre_pull(grad_normed)
    grad_input = grad_middle + grad_pre_part
    vectors = lax.psum(
        jnp.stack(
            [grad_pre_gain, grad_pre_shift, grad_b_out, grad_mid_gain, grad_mid_shift, grad_b_down]
            + [grad_b_up[j] for j in range(parts)],
            0,
        ),
        ("dp", "mp"),
    )
    g_b_up = lax.dynamic_slice_in_dim(vectors[6:], rank, 1, 0)[0]
    return (
        layer_out,
        grad_input,
        grad_first,
        vectors[0],
        vectors[1],
        grad_w_query.astype(f32),
        grad_b_query,
        grad_w_key.astype(f32),
        grad_w_value.astype(f32),
        grad_b_value,
        g_w_out,
        vectors[2],
        vectors[3],
        vectors[4],
        g_w_up,
        g_b_up,
        g_w_down,
        vectors[5],
    )


def tt(weight, rows):
    return lax.dot_general(weight, rows, (((0,), (1,)), ((), ())), preferred_element_type=jnp.float32)


def tt_rows(grad_t, weight):
    return lax.dot_general(grad_t, weight, (((0,), (1,)), ((), ())), preferred_element_type=jnp.float32)


def tn_t(rows, grad_t):
    return lax.dot_general(rows, grad_t, (((0,), (1,)), ((), ())), preferred_element_type=jnp.float32)


def solution(mesh):
    placed = (
        P(("dp", "mp"), None),
        P("dp", "mp"),
        P("dp"),
        P(),
        P(),
        P(None, "mp"),
        P("mp"),
        P(None, "mp"),
        P(None, "mp"),
        P("mp"),
        P("mp", None),
        P(),
        P(),
        P(),
        P(None, "mp"),
        P("mp"),
        P("mp", None),
        P(),
        P(("dp", "mp"), None),
    )
    return jax.shard_map(
        shards,
        mesh=mesh,
        in_specs=placed,
        out_specs=(
            P(("dp", "mp"), None),
            P(("dp", "mp"), None),
            P("dp", "mp"),
            P(),
            P(),
            P(None, "mp"),
            P("mp"),
            P(None, "mp"),
            P(None, "mp"),
            P("mp"),
            P("mp", None),
            P(),
            P(),
            P(),
            P(None, "mp"),
            P("mp"),
            P("mp", None),
            P(),
        ),
        check_vma=False,
    )
```
